256 devices in a mesh: samp: 32 (over z, y), pos: 8 (over x, core).
Axes of the slice: x: 4, y: 4, z: 8, core: 2. Of those that a mesh axis runs over, the one named last changes fastest.
Arguments:
- dosages: bfloat16 [65536, 4096], P('samp', 'pos')
- phenotypes: bfloat16 [65536, 2048], P('samp')
- gene_weights: bfloat16 [4096, 16], P('pos'), may hold values from -0.1875 to 0.1875
- gene_start: int32 [16], replicated, may hold values from 0 to 3072, as said below
- gene_end: int32 [16], replicated, may hold values from 1024 to 4096, as said below
Outputs:
- variant_z: float32 [2048, 4096], P('samp', 'pos')
- gene_z: float32 [2048, 16], P('samp', 'pos')
The draws below stay inside these ranges and needn't reach their ends.
Inputs may be any that keep to these rules, and one draw needn't show every extreme that they name: gene_end - gene_start lies between 1024 and 2048; some window starts at 0 and some ends at 4096. gene_end is greater than gene_start of the same gene.
All inputs are finite; a program needn't handle non-finite values.
Results may differ from the reference program's by a relative error of at most 0.0029.
Values sent between devices are 32-bit elements; how exact they have to be, the bound alone decides.
No kernel may reach another device: no remote copies, remote signals or barrier semaphores. Data moves between devices by JAX's collectives and lax.ppermute only.
A program may use at most 64 MiB of HBM per device.

```python
import jax
import jax.numpy as jnp
from jax import lax

VARIANTS = 4096
GENES = 16
TRAITS = 2048
SAMPLES = 65536


def scaled_rows(key, columns):
    rows = jnp.arange(SAMPLES, dtype=jnp.float32)
    rising = 1.0 + 2.0 * rows / SAMPLES
    base = jax.random.normal(key, (SAMPLES, columns), jnp.float32)
    return (base * rising[:, None]).astype(jnp.bfloat16)


def draw_dosages(key, part):
    return scaled_rows(jax.random.fold_in(key, 3), VARIANTS)


def draw_phenotypes(key, part):
    return scaled_rows(jax.random.fold_in(key, 5), TRAITS)


def window_pair(key):
    first_key, second_key = jax.random.split(jax.random.fold_in(key, 11))
    length = jax.random.randint(first_key, (GENES,), VARIANTS // 4, VARIANTS // 2 + 1)
    length = length.at[0].set(VARIANTS // 4)
    length = length.at[1].set(VARIANTS // 4)
    length = length.at[2].set(VARIANTS // 2)
    begin = jax.random.randint(second_key, (GENES,), 0, VARIANTS - length + 1)
    begin = begin.at[0].set(0)
    begin = begin.at[1].set(VARIANTS - length[1])
    return (begin.astype(jnp.int32), (begin + length).astype(jnp.int32))


def draw_gene_start(key, part):
    return window_pair(key)[0]


def draw_gene_end(key, part):
    return window_pair(key)[1]


def steps_of(own_key, extent, cuts, least, largest):
    level = 1.0
    for axis_at, blocks in cuts:
        draws = jax.random.uniform(jax.random.fold_in(jax.random.fold_in(own_key, 6), axis_at), (blocks,), jnp.float32, least / len(cuts), largest / len(cuts))
        level = level * jnp.repeat(jnp.exp(draws), extent[axis_at] // blocks).reshape((-1,) + (1,) * (len(extent) - 1 - axis_at))
    return level


def normal_values(own_key, shape, scale, bound, shards=(), kind=jnp.bfloat16):
    loudness = steps_of(own_key, shape, shards, -0.22, 0.18) if shards else 1.0
    result = jax.random.normal(own_key, shape, jnp.float32) * scale * loudness
    return jnp.minimum(jnp.maximum(result, -bound), bound).astype(kind)


def setup_inputs(seed: int = 0) -> dict:
    streams_of = jax.random.split(jax.random.key(seed), 6)
    return {
        "dosages": draw_dosages(jax.random.fold_in(streams_of[5], 71), 0),
        "phenotypes": draw_phenotypes(jax.random.fold_in(streams_of[5], 71), 0),
        "gene_weights": normal_values(streams_of[2], (VARIANTS, GENES), (VARIANTS // 4) ** -0.5, 0.1875, ((0, 8),)),
        "gene_start": draw_gene_start(jax.random.fold_in(streams_of[5], 71), 0),
        "gene_end": draw_gene_end(jax.random.fold_in(streams_of[5], 71), 0),
    }


EPSILON = 1e-06

def contract(left, right):
    return lax.dot_general(left, right, (((0,), (0,)), ((), ())), preferred_element_type=jnp.float32)

def reference(dosages, phenotypes, gene_weights, gene_start, gene_end):
    position = jnp.arange(VARIANTS, dtype=jnp.int32)[:, None]
    inside = (position >= gene_start[None, :]) & (position < gene_end[None, :])
    masked = jnp.where(inside, gene_weights, jnp.zeros_like(gene_weights))
    predicted = jnp.dot(dosages, masked, preferred_element_type=jnp.float32)
    pred_low = predicted.astype(jnp.bfloat16)
    marginal = contract(phenotypes, dosages)
    gene_cross = contract(phenotypes, pred_low)
    mean_dose = lax.optimization_barrier(jnp.sum(jnp.square(dosages.astype(jnp.float32)), axis=0)) / SAMPLES
    mean_trait = lax.optimization_barrier(jnp.sum(jnp.square(phenotypes.astype(jnp.float32)), axis=0)) / SAMPLES
    mean_pred = lax.optimization_barrier(jnp.sum(predicted * predicted, axis=0)) / SAMPLES
    variant_z = marginal / jnp.sqrt(SAMPLES * (mean_trait[:, None] + EPSILON) * (mean_dose[None, :] + EPSILON))
    gene_z = gene_cross / jnp.sqrt(SAMPLES * (mean_trait[:, None] + EPSILON) * (mean_pred[None, :] + EPSILON))
    return (variant_z, gene_z)
```

```python
import jax
import jax.numpy as jnp
from jax import lax
from jax.sharding import Mesh
from jax.sharding import PartitionSpec as P

SAMP = ("samp_0", "samp_1")
EPSILON = 1e-06


def contract(left, right):
    return lax.dot_general(
        left, right, (((0,), (0,)), ((), ())), preferred_element_type=jnp.float32
    )


def shifted(x, axis, by):
    count = lax.axis_size(axis)
    return lax.ppermute(x, axis, [(i, (i + by) % count) for i in range(count)])


def swapped(x, axis):
    return lax.all_to_all(x, axis, split_axis=0, concat_axis=0, tiled=True)


def per_device(dosages, phenotypes, gene_weights, gene_start, gene_end):
    width, gene_count = gene_weights.shape
    groups, ranks, spots = (lax.axis_size(a) for a in ("samp_0", "samp_1", "pos"))
    z, y = lax.axis_index("samp_0"), lax.axis_index("samp_1")
    samples = dosages.shape[0] * groups * ranks
    traits = phenotypes.shape[1]
    band = traits // groups
    own = band // ranks
    half = width // 2
    mine = gene_count // spots

    def band_at(k):
        return lax.rem(z + k + groups, groups)

    def z_block(k):
        cols = lax.dynamic_slice_in_dim(phenotypes, band_at(k) * band, band, 1)
        return contract(cols, dosages[:, :half])

    low = contract(phenotypes[:, : traits // 2], dosages[:, half:])
    high = contract(phenotypes[:, traits // 2 :], dosages[:, half:])
    low = low.reshape(groups // 2, ranks, own, half)
    high = high.reshape(groups // 2, ranks, own, half)

    def y_pick(part, k):
        return lax.dynamic_index_in_dim(part, lax.rem(y + k + ranks, ranks), 1, False)

    right = shifted(y_pick(low, 2), "samp_1", 1)
    left = shifted(y_pick(high, 2), "samp_1", -1)
    z4 = z_block(4)
    zr = shifted(z4[: band // 2], "samp_0", 1)
    zl = shifted(z4[band // 2 :], "samp_0", -1)

    offset = lax.axis_index("pos") * width
    position = offset + lax.broadcasted_iota(jnp.int32, (width, gene_count), 0)
    inside = (position >= gene_start[None, :]) & (position < gene_end[None, :])
    masked = jnp.where(inside, gene_weights, jnp.zeros_like(gene_weights))
    partial_value = lax.dot_general(
        masked, dosages, (((0,), (1,)), ((), ())), preferred_element_type=jnp.float32
    )
    predicted = swapped(partial_value.reshape(spots, mine, -1), "pos").sum(axis=0)
    pred_low = predicted.astype(jnp.bfloat16)
    cross = lax.dot_general(
        pred_low, phenotypes, (((1,), (0,)), ((), ())), preferred_element_type=jnp.float32
    )
    pred_sq = jnp.sum(predicted * predicted, axis=1)
    dose_sq = jnp.sum(jnp.square(dosages.astype(jnp.float32)), axis=0)
    trait_sq = jnp.sum(jnp.square(phenotypes.astype(jnp.float32)), axis=0)
    per_owner = [
        jnp.broadcast_to(dose_sq, (groups * ranks, width)),
        cross.reshape(mine, groups * ranks, own).transpose(1, 0, 2).reshape(groups * ranks, mine * own),
        trait_sq.reshape(groups * ranks, own),
        jnp.broadcast_to(jnp.pad(pred_sq, (0, 62)), (groups * ranks, 64)),
    ]
    extra = jnp.concatenate(per_owner, axis=1).reshape(groups, ranks, 3, half)
    extra = extra.transpose(1, 0, 2, 3).reshape(ranks, groups * 3, half)
    extra = swapped(extra, "samp_1").sum(axis=0).reshape(groups, 3, half)

    right = shifted(
        jnp.concatenate([y_pick(low, 1) + right, y_pick(high, 1)], 0), "samp_1", 1
    )
    left = shifted(
        jnp.concatenate([y_pick(low, -1), y_pick(high, -1) + left], 0), "samp_1", -1
    )
    z3, zm3 = z_block(3), z_block(-3)
    zr = shifted(jnp.concatenate([z3[: band // 2] + zr, z3[band // 2 :]], 0), "samp_0", 1)
    zl = shifted(jnp.concatenate([zm3[: band // 2], zm3[band // 2 :] + zl], 0), "samp_0", -1)
    for k in (2, 1):
        zr = shifted(z_block(k) + zr, "samp_0", 1)
        zl = shifted(z_block(-k) + zl, "samp_0", -1)
    first = z_block(0) + zr + zl
    first = swapped(first.reshape(ranks, own, half), "samp_1").sum(axis=0)

    second = jnp.concatenate([y_pick(low, 0), y_pick(high, 0)], 0) + right + left
    second = jnp.concatenate([second, jnp.pad(extra, ((0, 0), (0, 5), (0, 0)))], 1)
    second = swapped(second, "samp_0").sum(axis=0)

    mean_dose = second[own : own + 2].reshape(width) / samples
    rest = second[own + 2]
    gene_cross = rest[: mine * own].reshape(mine, own).T
    mean_trait = rest[mine * own : mine * own + own] / samples
    mean_pred = rest[mine * own + own : mine * own + own + mine] / samples
    marginal = jnp.concatenate([first, second[:own]], 1)
    variant_z = marginal / jnp.sqrt(
        samples * (mean_trait[:, None] + EPSILON) * (mean_dose[None, :] + EPSILON)
    )
    gene_z = gene_cross / jnp.sqrt(
        samples * (mean_trait[:, None] + EPSILON) * (mean_pred[None, :] + EPSILON)
    )
    return (variant_z, gene_z)


def solution(mesh):
    finer = Mesh(mesh.devices.reshape(8, 4, mesh.shape["pos"]), ("samp_0", "samp_1", "pos"))
    in_specs = (P(SAMP, "pos"), P(SAMP, None), P("pos", None), P(), P())
    out_specs = (P(SAMP, "pos"), P(SAMP, "pos"))
    return jax.shard_map(
        per_device, mesh=finer, in_specs=in_specs, out_specs=out_specs, check_vma=False
    )
```

```python
import jax
import jax.numpy as jnp
from jax import lax
from jax.experimental import pallas as pl
from jax.experimental.pallas import tpu as pltpu
from jax.sharding import Mesh
from jax.sharding import PartitionSpec as P


SAMP = ("samp_0", "samp_1")
EPSILON = 1e-06
CUT = 40


def contract(left, right):
    return lax.dot_general(
        left, right, (((0,), (0,)), ((), ())), preferred_element_type=jnp.float32
    )


def shifted(x, axis, by):
    count = lax.axis_size(axis)
    return lax.ppermute(x, axis, [(i, (i + by) % count) for i in range(count)])


def parted(x, axis):
    count, spots = lax.axis_size(axis), lax.axis_size("pos")
    pairs = []
    for i in range(count):
        for p in range(spots):
            to = (i + (1 if p % 2 == 0 else -1)) % count
            pairs.append((i * spots + p, to * spots + p))
    return lax.ppermute(x, (axis, "pos"), pairs)


def swapped(x, axis):
    return lax.all_to_all(x, axis, split_axis=0, concat_axis=0, tiled=True)


def far_product(place, phenotypes, dosages, groups, ranks):
    depth, traits = phenotypes.shape
    width = dosages.shape[1]
    band = traits // groups
    own = band // ranks

    def body(place, p_ref, d_ref, o_ref, f_ref):
        both = contract(p_ref[...], d_ref[...])
        o_ref[...] = both
        for r in range(ranks):
            f_ref[r] = both[r * own : r * own + CUT]

    return pl.pallas_call(
        body,
        grid_spec=pltpu.PrefetchScalarGridSpec(
            num_scalar_prefetch=1,
            grid=(1,),
            in_specs=[
                pl.BlockSpec((depth, band), lambda i, place: (0, lax.rem(place[0] + groups // 2, groups))),
                pl.BlockSpec((depth, width), lambda i, place: (0, 0)),
            ],
            out_specs=[
                pl.BlockSpec((band, width), lambda i, place: (0, 0)),
                pl.BlockSpec((ranks, CUT, width), lambda i, place: (0, 0, 0)),
            ],
        ),
        out_shape=[
            jax.ShapeDtypeStruct((band, width), jnp.float32),
            jax.ShapeDtypeStruct((ranks, CUT, width), jnp.float32),
        ],
        compiler_params=pltpu.CompilerParams(vmem_limit_bytes=56 * 2**20),
        cost_estimate=pl.CostEstimate(
            flops=2 * depth * band * width, bytes_accessed=2 * depth * (band + width), transcendentals=0
        ),
        name="far_product",
    )(place[0], phenotypes, dosages)


def products(far, place, phenotypes, dosages, weights, begin, end, groups, ranks, spots):
    depth, traits = phenotypes.shape
    genes, width = weights.shape
    mine = genes // spots
    band = traits // groups
    own = band // ranks
    rest = own - CUT

    def at(i, place):
        k = jnp.where(i % 2 == 1, groups // 2 - (i + 1) // 2, i // 2 + groups // 2)
        return lax.rem(place[0] + k, groups)

    def body(place, spot, turn, first, last, c_ref, p_ref, d_ref, w_ref, y0_ref, y1_ref, y2_ref, y3_ref, z_ref, t_ref, q_ref, g_ref, held, blocks, low_w, sems):
        i = pl.program_id(0)

        def fetch(step):
            cols = pl.ds(pl.multiple_of(at(step, place) * band, band), band)
            slot = step % 2
            return pltpu.make_async_copy(p_ref.at[:, cols], blocks.at[slot], sems.at[slot])

        @pl.when(i == 0)
        def _():
            fetch(i).start()

        @pl.when(i + 1 < groups)
        def _():
            fetch(i + 1).start()

        @pl.when(i == 0)
        def _():
            d = d_ref[...].astype(jnp.float32)
            q_ref[...] = jnp.sum(d * d, axis=0, keepdims=True)
            gene = lax.broadcasted_iota(jnp.int32, (genes, width), 0)
            position = spot[0] * width + lax.broadcasted_iota(jnp.int32, (genes, width), 1)
            low, high = jnp.zeros_like(gene), jnp.zeros_like(gene)
            for g in range(genes):
                low = jnp.where(gene == g, first[g], low)
                high = jnp.where(gene == g, last[g], high)
            w = w_ref[...].astype(jnp.float32)
            w = jnp.where((position >= low) & (position < high), w, 0.0).astype(jnp.bfloat16)
            value = lax.dot_general(
                w, d_ref[...], (((1,), (1,)), ((), ())), preferred_element_type=jnp.float32
            )
            low_w[...] = w
            for s in range(spots):
                g_ref[s, :mine] = value[s * mine : (s + 1) * mine, :]

        fetch(i).wait()
        here = blocks[i % 2]

        @pl.when(i == 0)
        def _():
            held[...] = c_ref[...]

        @pl.when(i > 0)
        def _():
            held[...] = contract(here, d_ref[...])

        both = held[...]
        upper = both.astype(jnp.bfloat16)
        lower = (both - upper.astype(jnp.float32)).astype(jnp.bfloat16)
        cross = sum(
            lax.dot_general(low_w[...], part, (((1,), (1,)), ((), ())), preferred_element_type=jnp.float32)
            for part in (upper, lower)
        )
        cols = pl.ds(pl.multiple_of(at(i, place) * band, band), band)
        for s in range(spots):
            g_ref[s, mine:, cols] = cross[s * mine : (s + 1) * mine, :]

        @pl.when(pl.program_id(0) > 0)
        def _():
            for r in range(ranks):
                z_ref[0, r] = held[r * own : r * own + CUT, :]

        for k, out in enumerate((y0_ref, y1_ref, y2_ref, y3_ref)):
            start = lax.rem(turn[0] + k, ranks) * own + CUT
            out[0] = held[pl.ds(pl.multiple_of(start, 8), rest), :]
        p = here.astype(jnp.float32)
        t_ref[...] = jnp.sum(p * p, axis=0, keepdims=True)

    whole = lambda i, place, *_: (0, 0)
    piece = jax.ShapeDtypeStruct((groups, rest, width), jnp.float32)
    return pl.pallas_call(
        body,
        grid_spec=pltpu.PrefetchScalarGridSpec(
            num_scalar_prefetch=5,
            grid=(groups,),
            in_specs=[
                pl.BlockSpec((band, width), whole),
                pl.BlockSpec(memory_space=pltpu.HBM),
                pl.BlockSpec((depth, width), whole),
                pl.BlockSpec((genes, width), whole),
            ],
            out_specs=[pl.BlockSpec((1, rest, width), lambda i, place, *_: (at(i, place), 0, 0))] * ranks
            + [
                pl.BlockSpec((1, ranks, CUT, width), lambda i, place, *_: (jnp.maximum(i - 1, 0), 0, 0, 0)),
                pl.BlockSpec((1, band), lambda i, place, *_: (0, at(i, place))),
                pl.BlockSpec((1, width), whole),
                pl.BlockSpec((spots, 2 * mine, depth), lambda i, place, *_: (0, 0, 0)),
            ],
            scratch_shapes=[
                pltpu.VMEM((band, width), jnp.float32),
                pltpu.VMEM((2, depth, band), jnp.bfloat16),
                pltpu.VMEM((genes, width), jnp.bfloat16),
                pltpu.SemaphoreType.DMA((2,)),
            ],
        ),
        out_shape=[piece] * ranks
        + [
            jax.ShapeDtypeStruct((groups - 1, ranks, CUT, width), jnp.float32),
            jax.ShapeDtypeStruct((1, traits), jnp.float32),
            jax.ShapeDtypeStruct((1, width), jnp.float32),
            jax.ShapeDtypeStruct((spots, 2 * mine, depth), jnp.float32),
        ],
        compiler_params=pltpu.CompilerParams(vmem_limit_bytes=56 * 2**20),
        cost_estimate=pl.CostEstimate(
            flops=2 * depth * traits * width, bytes_accessed=2 * depth * (traits + width), transcendentals=0
        ),
        name="products",
    )(place[0], place[2], place[1], begin, end, far, phenotypes, dosages, weights)


def small_sums(parts, trait_sq, dose_sq, groups):
    spots, rows, _ = parts.shape
    mine = rows // 2
    band = trait_sq.shape[1] // groups
    width = dose_sq.shape[1]

    def body(g_ref, t_ref, q_ref, o_ref):
        total = g_ref[0]
        for s in range(1, spots):
            total = total + g_ref[s]
        predicted = total[:mine]
        squares = jnp.sum(predicted * predicted, axis=1, keepdims=True)
        o_ref[...] = jnp.zeros_like(o_ref)
        for g in range(groups):
            cols = slice(g * band, (g + 1) * band)
            o_ref[8 * g : 8 * g + mine, :band] = total[mine:, cols]
            o_ref[8 * g + 2 : 8 * g + 3, :band] = t_ref[:, cols]
            o_ref[8 * g + 3 : 8 * g + 4, :] = q_ref[...]
            o_ref[8 * g + 4 : 8 * g + 4 + mine, :] = jnp.broadcast_to(squares, (mine, width))

    return pl.pallas_call(
        body,
        out_shape=jax.ShapeDtypeStruct((8 * groups, width), jnp.float32),
        compiler_params=pltpu.CompilerParams(vmem_limit_bytes=8 * 2**20),
        cost_estimate=pl.CostEstimate(flops=10**6, bytes_accessed=10**6, transcendentals=0),
        name="small_sums",
    )(parts, trait_sq, dose_sq)


def joined(pieces, extras):
    groups, rest, width = pieces[0].shape
    count = len(pieces)

    def body(*refs):
        o_ref = refs[-1]
        total = refs[0][...]
        for ref in refs[1:count]:
            total = total + ref[...]
        o_ref[:, :rest, :] = total
        small = refs[count][...]
        for ref in refs[count + 1 : -1]:
            small = small + ref[...]
        for g in range(groups):
            o_ref[g, rest:, :] = small[8 * g : 8 * g + 8, :]

    return pl.pallas_call(
        body,
        out_shape=jax.ShapeDtypeStruct((groups, rest + 8, width), jnp.float32),
        compiler_params=pltpu.CompilerParams(vmem_limit_bytes=16 * 2**20),
        cost_estimate=pl.CostEstimate(
            flops=count * pieces[0].size, bytes_accessed=20 * pieces[0].size, transcendentals=0
        ),
        name="joined",
    )(*pieces, *extras)


def device_part(dosages, phenotypes, gene_weights, gene_start, gene_end):
    _, gene_count = gene_weights.shape
    groups, ranks, spots = (lax.axis_size(a) for a in ("samp_0", "samp_1", "pos"))
    z, y, x = (lax.axis_index(a) for a in ("samp_0", "samp_1", "pos"))
    samples = dosages.shape[0] * groups * ranks
    traits = phenotypes.shape[1]
    band = traits // groups
    own = band // ranks
    rest = own - CUT
    mine = gene_count // spots
    forward = lax.rem(x, 2) == 0

    place = (z.reshape(1), y.reshape(1), x.reshape(1))
    far, z_far = far_product(place, phenotypes, dosages, groups, ranks)
    z_in = parted(z_far, "samp_0")
    y0, y1, y2, y3, z_own, trait_sq, dose_sq, partial_value = products(
        far, place, phenotypes, dosages, gene_weights.T, gene_start, gene_end, groups, ranks, spots
    )
    arrived = [shifted(y2, "samp_1", 2), shifted(y1, "samp_1", 1), shifted(y3, "samp_1", -1)]
    parts = swapped(partial_value, "pos")

    nothing = jnp.zeros_like(z_in)
    z_right = shifted(z_own[0] + jnp.where(forward, z_in, nothing), "samp_0", 1)
    z_left = shifted(z_own[1] + jnp.where(forward, nothing, z_in), "samp_0", -1)

    extra = small_sums(parts, trait_sq, dose_sq, groups)
    extras = [extra] + [shifted(extra, "samp_1", k) for k in (2, 1, 3)]

    for at in (2, 4):
        z_right, z_left = lax.optimization_barrier((z_right, z_left))
        z_right = shifted(z_own[at] + z_right, "samp_0", 1)
        z_left = shifted(z_own[at + 1] + z_left, "samp_0", -1)

    second = joined([y0] + arrived, extras)
    second = swapped(second, "samp_0").sum(axis=0)

    first = z_own[6] + z_right + z_left

    def for_rank(k):
        return lax.dynamic_index_in_dim(first, lax.rem(y + k, ranks), 0, False)

    first = for_rank(0) + sum(shifted(for_rank(k), "samp_1", k) for k in (2, 1, 3))

    small = second[rest:]
    mean_dose = small[3] / samples
    mean_pred = small[4 : 4 + mine, 0] / samples
    here = lax.dynamic_slice_in_dim(small[: mine + 1], y * own, own, 1)
    gene_cross = here[:mine].T
    mean_trait = here[mine] / samples
    marginal = jnp.concatenate([first, second[:rest]], 0)
    variant_z = marginal / jnp.sqrt(
        samples * (mean_trait[:, None] + EPSILON) * (mean_dose[None, :] + EPSILON)
    )
    gene_z = gene_cross / jnp.sqrt(
        samples * (mean_trait[:, None] + EPSILON) * (mean_pred[None, :] + EPSILON)
    )
    return (variant_z, gene_z)


def solution(mesh):
    finer = Mesh(mesh.devices.reshape(8, 4, mesh.shape["pos"]), ("samp_0", "samp_1", "pos"))
    in_specs = (P(SAMP, "pos"), P(SAMP, None), P("pos", None), P(), P())
    out_specs = (P(SAMP, "pos"), P(SAMP, "pos"))
    return jax.shard_map(device_part, mesh=finer, in_specs=in_specs, out_specs=out_specs, check_vma=False)
```

```python
import jax
import jax.numpy as jnp
from jax import lax
from jax.experimental import pallas as pl
from jax.experimental.pallas import tpu as pltpu
from jax.sharding import Mesh
from jax.sharding import PartitionSpec as P


SAMP = ("samp_0", "samp_1")
EPSILON = 1e-06
CUT = 48


def contract(left, right):
    return lax.dot_general(
        left, right, (((0,), (0,)), ((), ())), preferred_element_type=jnp.float32
    )


def shifted(x, axis, by):
    count = lax.axis_size(axis)
    return lax.ppermute(x, axis, [(i, (i + by) % count) for i in range(count)])


def parted(x, axis):
    count, spots = lax.axis_size(axis), lax.axis_size("pos")
    pairs = []
    for i in range(count):
        for p in range(spots):
            to = (i + (1 if p % 2 == 0 else -1)) % count
            pairs.append((i * spots + p, to * spots + p))
    return lax.ppermute(x, (axis, "pos"), pairs)


def swapped(x, axis):
    return lax.all_to_all(x, axis, split_axis=0, concat_axis=0, tiled=True)


def far_product(place, phenotypes, dosages, groups, ranks):
    depth, traits = phenotypes.shape
    width = dosages.shape[1]
    band = traits // groups
    own = band // ranks

    def body(place, p_ref, d_ref, o_ref, f_ref, q_ref):
        d = d_ref[...].astype(jnp.float32)
        q_ref[...] = jnp.sum(d * d, axis=0, keepdims=True)
        both = contract(p_ref[...], d_ref[...])
        o_ref[...] = both
        for r in range(ranks):
            f_ref[r] = both[r * own : r * own + CUT]

    return pl.pallas_call(
        body,
        grid_spec=pltpu.PrefetchScalarGridSpec(
            num_scalar_prefetch=1,
            grid=(1,),
            in_specs=[
                pl.BlockSpec((depth, band), lambda i, place: (0, lax.rem(place[0] + groups // 2, groups))),
                pl.BlockSpec((depth, width), lambda i, place: (0, 0)),
            ],
            out_specs=[
                pl.BlockSpec((band, width), lambda i, place: (0, 0)),
                pl.BlockSpec((ranks, CUT, width), lambda i, place: (0, 0, 0)),
                pl.BlockSpec((1, width), lambda i, place: (0, 0)),
            ],
        ),
        out_shape=[
            jax.ShapeDtypeStruct((band, width), jnp.float32),
            jax.ShapeDtypeStruct((ranks, CUT, width), jnp.float32),
            jax.ShapeDtypeStruct((1, width), jnp.float32),
        ],
        compiler_params=pltpu.CompilerParams(vmem_limit_bytes=56 * 2**20),
        cost_estimate=pl.CostEstimate(
            flops=2 * depth * band * width, bytes_accessed=2 * depth * (band + width), transcendentals=0
        ),
        name="far_product",
    )(place[0], phenotypes, dosages)


def products(rel, far, earlier, place, phenotypes, dosages, weights, begin, end, groups, ranks, spots):
    depth, traits = phenotypes.shape
    genes, width = weights.shape
    mine = genes // spots
    band = traits // groups
    own = band // ranks
    rest = own - CUT
    count, copied = len(rel), far is not None
    kept = count - 1 if copied else count

    def at(i, place):
        k = sum(jnp.where(i == j, d + groups, 0) for j, d in enumerate(rel))
        return lax.rem(place[0] + k, groups)

    def now(i):
        return jnp.minimum(i, count - 1)

    def before(i):
        return jnp.maximum(i - 1, 0)

    def body(place, spot, turn, first, last, p_ref, d_ref, w_ref, *refs):
        if copied:
            c_ref, refs = refs[0], refs[1:]
        if earlier is not None:
            refs = refs[ranks + 2 :]
        y_refs, (t_ref, g_ref, z_ref, even, odd, low_w) = refs[:ranks], refs[ranks:]
        i = pl.program_id(0)

        def multiply(to):
            to[...] = contract(p_ref[...], d_ref[...])

        def squares():
            p = p_ref[...].astype(jnp.float32)
            t_ref[...] = jnp.sum(p * p, axis=0, keepdims=True)

        def store(held, keep):
            both = held[...]
            if keep:
                for r in range(ranks):
                    z_ref[0, r] = both[r * own : r * own + CUT, :]
            for k, out in enumerate(y_refs):
                start = lax.rem(turn[0] + k, ranks) * own + CUT
                out[0] = held[pl.ds(pl.multiple_of(start, 8), rest), :]
            upper = both.astype(jnp.bfloat16)
            lower = (both - upper.astype(jnp.float32)).astype(jnp.bfloat16)
            rows = pl.ds(pl.multiple_of(at(before(i), place) * band, band), band)
            w = low_w[...]
            value = lax.dot_general(
                w, d_ref[rows, :], (((1,), (1,)), ((), ())), preferred_element_type=jnp.float32
            )
            cross = sum(
                lax.dot_general(w, part, (((1,), (1,)), ((), ())), preferred_element_type=jnp.float32)
                for part in (upper, lower)
            )
            for s in range(spots):
                g_ref[s, :mine] = value[s * mine : (s + 1) * mine, :]
                g_ref[s, mine:] = cross[s * mine : (s + 1) * mine, :]

        @pl.when(i == 0)
        def _():
            gene = lax.broadcasted_iota(jnp.int32, (genes, width), 0)
            position = spot[0] * width + lax.broadcasted_iota(jnp.int32, (genes, width), 1)
            low, high = jnp.zeros_like(gene), jnp.zeros_like(gene)
            for g in range(genes):
                low = jnp.where(gene == g, first[g], low)
                high = jnp.where(gene == g, last[g], high)
            w = w_ref[...].astype(jnp.float32)
            low_w[...] = jnp.where((position >= low) & (position < high), w, 0.0).astype(jnp.bfloat16)
            if copied:
                even[...] = c_ref[...]
            else:
                multiply(even)
            squares()

        if copied:

            @pl.when(i == 1)
            def _():
                multiply(odd)
                store(even, False)
                squares()

        @pl.when((i % 2 == 1) & (i < count) & (i >= (3 if copied else 1)))
        def _():
            multiply(odd)
            store(even, True)
            squares()

        @pl.when((i % 2 == 0) & (i < count) & (i > 0))
        def _():
            multiply(even)
            store(odd, True)
            squares()

        @pl.when(i == count)
        def _():
            store(odd if count % 2 == 0 else even, True)

    whole = lambda i, *_: (0, 0)
    in_specs = [
        pl.BlockSpec((depth, band), lambda i, place, *_: (0, at(now(i), place))),
        pl.BlockSpec((depth, width), whole),
        pl.BlockSpec((genes, width), whole),
    ]
    operands = [place[0], place[2], place[1], begin, end, phenotypes, dosages, weights]
    aliases = {}
    if copied:
        in_specs.append(pl.BlockSpec((band, width), whole))
        operands.append(far)
    if earlier is not None:
        aliases = {len(operands) + k: k for k in range(len(earlier))}
        in_specs += [pl.BlockSpec(memory_space=pl.ANY)] * len(earlier)
        operands += earlier
    return pl.pallas_call(
        body,
        grid_spec=pltpu.PrefetchScalarGridSpec(
            num_scalar_prefetch=5,
            grid=(count + 1,),
            in_specs=in_specs,
            out_specs=[pl.BlockSpec((1, rest, width), lambda i, place, *_: (at(before(i), place), 0, 0))] * ranks
            + [
                pl.BlockSpec((1, band), lambda i, place, *_: (0, at(now(i), place))),
                pl.BlockSpec((spots, 2 * mine, band), lambda i, place, *_: (0, 0, at(before(i), place))),
                pl.BlockSpec(
                    (1, ranks, CUT, width), lambda i, *_: (jnp.clip(i - 1 - count + kept, 0, kept - 1), 0, 0, 0)
                ),
            ],
            scratch_shapes=[
                pltpu.VMEM((band, width), jnp.float32),
                pltpu.VMEM((band, width), jnp.float32),
                pltpu.VMEM((genes, width), jnp.bfloat16),
            ],
        ),
        out_shape=[jax.ShapeDtypeStruct((groups, rest, width), jnp.float32)] * ranks
        + [
            jax.ShapeDtypeStruct((1, traits), jnp.float32),
            jax.ShapeDtypeStruct((spots, 2 * mine, depth), jnp.float32),
            jax.ShapeDtypeStruct((kept, ranks, CUT, width), jnp.float32),
        ],
        input_output_aliases=aliases,
        compiler_params=pltpu.CompilerParams(vmem_limit_bytes=56 * 2**20),
        cost_estimate=pl.CostEstimate(
            flops=2 * depth * band * count * width, bytes_accessed=2 * depth * (traits + width), transcendentals=0
        ),
        name="products",
    )(*operands)


def small_sums(parts, trait_sq, dose_sq, groups):
    spots, rows, _ = parts.shape
    mine = rows // 2
    band = trait_sq.shape[1] // groups
    width = dose_sq.shape[1]

    def body(g_ref, t_ref, q_ref, o_ref):
        total = g_ref[0]
        for s in range(1, spots):
            total = total + g_ref[s]
        predicted = total[:mine]
        squares = jnp.sum(predicted * predicted, axis=1, keepdims=True)
        o_ref[...] = jnp.zeros_like(o_ref)
        for g in range(groups):
            cols = slice(g * band, (g + 1) * band)
            o_ref[8 * g : 8 * g + mine, :band] = total[mine:, cols]
            o_ref[8 * g + 2 : 8 * g + 3, :band] = t_ref[:, cols]
            o_ref[8 * g + 3 : 8 * g + 4, :] = q_ref[...]
            o_ref[8 * g + 4 : 8 * g + 4 + mine, :] = jnp.broadcast_to(squares, (mine, width))

    return pl.pallas_call(
        body,
        out_shape=jax.ShapeDtypeStruct((8 * groups, width), jnp.float32),
        compiler_params=pltpu.CompilerParams(vmem_limit_bytes=8 * 2**20),
        cost_estimate=pl.CostEstimate(flops=10**6, bytes_accessed=10**6, transcendentals=0),
        name="small_sums",
    )(parts, trait_sq, dose_sq)


def joined(pieces, extras):
    groups, rest, width = pieces[0].shape
    count = len(pieces)

    def body(*refs):
        o_ref = refs[-1]
        total = refs[0][...]
        for ref in refs[1:count]:
            total = total + ref[...]
        o_ref[:, :rest, :] = total
        small = refs[count][...]
        for ref in refs[count + 1 : -1]:
            small = small + ref[...]
        for g in range(groups):
            o_ref[g, rest:, :] = small[8 * g : 8 * g + 8, :]

    return pl.pallas_call(
        body,
        out_shape=jax.ShapeDtypeStruct((groups, rest + 8, width), jnp.float32),
        compiler_params=pltpu.CompilerParams(vmem_limit_bytes=16 * 2**20),
        cost_estimate=pl.CostEstimate(
            flops=count * pieces[0].size, bytes_accessed=20 * pieces[0].size, transcendentals=0
        ),
        name="joined",
    )(*pieces, *extras)


def device_part(dosages, phenotypes, gene_weights, gene_start, gene_end):
    _, gene_count = gene_weights.shape
    groups, ranks, spots = (lax.axis_size(a) for a in ("samp_0", "samp_1", "pos"))
    z, y, x = (lax.axis_index(a) for a in ("samp_0", "samp_1", "pos"))
    samples = dosages.shape[0] * groups * ranks
    traits = phenotypes.shape[1]
    band = traits // groups
    own = band // ranks
    rest = own - CUT
    mine = gene_count // spots
    forward = lax.rem(x, 2) == 0

    place = (z.reshape(1), y.reshape(1), x.reshape(1))
    far, z_far, dose_sq = far_product(place, phenotypes, dosages, groups, ranks)
    z_in = parted(z_far, "samp_0")
    rest_of = (place, phenotypes, dosages, gene_weights.T, gene_start, gene_end, groups, ranks, spots)
    *earlier, z_own = products((3, -3, 2, -2), None, None, *rest_of)
    *earlier, z_last = products((4, 1, -1, 0), far, earlier, *rest_of)
    y0, y1, y2, y3, trait_sq, partial_value = earlier
    arrived = [shifted(y2, "samp_1", 2), shifted(y1, "samp_1", 1), shifted(y3, "samp_1", -1)]
    parts = swapped(partial_value, "pos")

    nothing = jnp.zeros_like(z_in)
    z_right = shifted(z_own[0] + jnp.where(forward, z_in, nothing), "samp_0", 1)
    z_left = shifted(z_own[1] + jnp.where(forward, nothing, z_in), "samp_0", -1)

    extra = small_sums(parts, trait_sq, dose_sq, groups)
    extras = [extra] + [shifted(extra, "samp_1", k) for k in (2, 1, 3)]

    for mid in (z_own[2:], z_last):
        z_right, z_left = lax.optimization_barrier((z_right, z_left))
        z_right = shifted(mid[0] + z_right, "samp_0", 1)
        z_left = shifted(mid[1] + z_left, "samp_0", -1)

    second = joined([y0] + arrived, extras)
    second = swapped(second, "samp_0").sum(axis=0)

    first = z_last[2] + z_right + z_left

    def for_rank(k):
        return lax.dynamic_index_in_dim(first, lax.rem(y + k, ranks), 0, False)

    first = for_rank(0) + sum(shifted(for_rank(k), "samp_1", k) for k in (2, 1, 3))

    small = second[rest:]
    mean_dose = small[3] / samples
    mean_pred = small[4 : 4 + mine, 0] / samples
    here = lax.dynamic_slice_in_dim(small[: mine + 1], y * own, own, 1)
    gene_cross = here[:mine].T
    mean_trait = here[mine] / samples
    marginal = jnp.concatenate([first, second[:rest]], 0)
    variant_z = marginal / jnp.sqrt(
        samples * (mean_trait[:, None] + EPSILON) * (mean_dose[None, :] + EPSILON)
    )
    gene_z = gene_cross / jnp.sqrt(
        samples * (mean_trait[:, None] + EPSILON) * (mean_pred[None, :] + EPSILON)
    )
    return (variant_z, gene_z)


def solution(mesh):
    finer = Mesh(mesh.devices.reshape(8, 4, mesh.shape["pos"]), ("samp_0", "samp_1", "pos"))
    in_specs = (P(SAMP, "pos"), P(SAMP, None), P("pos", None), P(), P())
    out_specs = (P(SAMP, "pos"), P(SAMP, "pos"))
    return jax.shard_map(device_part, mesh=finer, in_specs=in_specs, out_specs=out_specs, check_vma=False)
```

```python
import jax
import jax.numpy as jnp
from jax import lax
from jax.experimental import pallas as pl
from jax.experimental.pallas import tpu as pltpu
from jax.sharding import Mesh
from jax.sharding import PartitionSpec as P


SAMP = ("samp_0", "samp_1")
EPSILON = 1e-06
CUT = 56


def contract(left, right):
    return lax.dot_general(
        left, right, (((0,), (0,)), ((), ())), preferred_element_type=jnp.float32
    )


def shifted(x, axis, by):
    count = lax.axis_size(axis)
    return lax.ppermute(x, axis, [(i, (i + by) % count) for i in range(count)])


def parted(x, axis):
    count, spots = lax.axis_size(axis), lax.axis_size("pos")
    pairs = []
    for i in range(count):
        for p in range(spots):
            to = (i + (1 if p % 2 == 0 else -1)) % count
            pairs.append((i * spots + p, to * spots + p))
    return lax.ppermute(x, (axis, "pos"), pairs)


def swapped(x, axis):
    return lax.all_to_all(x, axis, split_axis=0, concat_axis=0, tiled=True)


def far_product(place, phenotypes, dosages, groups, ranks):
    depth, traits = phenotypes.shape
    width = dosages.shape[1]
    band = traits // groups
    own = band // ranks

    def body(place, p_ref, d_ref, o_ref, f_ref, q_ref):
        d = d_ref[...].astype(jnp.float32)
        q_ref[...] = jnp.sum(d * d, axis=0, keepdims=True)
        both = contract(p_ref[...], d_ref[...])
        o_ref[...] = both
        for r in range(ranks):
            f_ref[r] = both[r * own : r * own + CUT]

    return pl.pallas_call(
        body,
        grid_spec=pltpu.PrefetchScalarGridSpec(
            num_scalar_prefetch=1,
            grid=(1,),
            in_specs=[
                pl.BlockSpec((depth, band), lambda i, place: (0, lax.rem(place[0] + groups // 2, groups))),
                pl.BlockSpec((depth, width), lambda i, place: (0, 0)),
            ],
            out_specs=[
                pl.BlockSpec((band, width), lambda i, place: (0, 0)),
                pl.BlockSpec((ranks, CUT, width), lambda i, place: (0, 0, 0)),
                pl.BlockSpec((1, width), lambda i, place: (0, 0)),
            ],
        ),
        out_shape=[
            jax.ShapeDtypeStruct((band, width), jnp.float32),
            jax.ShapeDtypeStruct((ranks, CUT, width), jnp.float32),
            jax.ShapeDtypeStruct((1, width), jnp.float32),
        ],
        compiler_params=pltpu.CompilerParams(vmem_limit_bytes=56 * 2**20),
        cost_estimate=pl.CostEstimate(
            flops=2 * depth * band * width, bytes_accessed=2 * depth * (band + width), transcendentals=0
        ),
        name="far_product",
    )(place[0], phenotypes, dosages)


def products(rel, far, earlier, place, phenotypes, dosages, weights, begin, end, groups, ranks, spots):
    depth, traits = phenotypes.shape
    genes, width = weights.shape
    mine = genes // spots
    band = traits // groups
    own = band // ranks
    rest = own - CUT
    count, copied = len(rel), far is not None
    kept = count - 1 if copied else count

    def at(i, place):
        k = sum(jnp.where(i == j, d + groups, 0) for j, d in enumerate(rel))
        return lax.rem(place[0] + k, groups)

    def now(i):
        return jnp.minimum(i, count - 1)

    def before(i):
        return jnp.maximum(i - 1, 0)

    def body(place, spot, turn, first, last, p_ref, d_ref, w_ref, *refs):
        if copied:
            c_ref, refs = refs[0], refs[1:]
        if earlier is not None:
            refs = refs[ranks + 2 :]
        y_refs, (t_ref, g_ref, z_ref, even, odd, low_w) = refs[:ranks], refs[ranks:]
        i = pl.program_id(0)

        def multiply(to):
            to[...] = contract(p_ref[...], d_ref[...])

        def squares():
            p = p_ref[...].astype(jnp.float32)
            t_ref[...] = jnp.sum(p * p, axis=0, keepdims=True)

        def store(held, keep):
            both = held[...]
            if keep:
                for r in range(ranks):
                    z_ref[0, r] = both[r * own : r * own + CUT, :]
            for k, out in enumerate(y_refs):
                start = lax.rem(turn[0] + k, ranks) * own + CUT
                out[0] = held[pl.ds(pl.multiple_of(start, 8), rest), :]
            upper = both.astype(jnp.bfloat16)
            lower = (both - upper.astype(jnp.float32)).astype(jnp.bfloat16)
            rows = pl.ds(pl.multiple_of(at(before(i), place) * band, band), band)
            w = low_w[...]
            value = lax.dot_general(
                w, d_ref[rows, :], (((1,), (1,)), ((), ())), preferred_element_type=jnp.float32
            )
            cross = sum(
                lax.dot_general(w, part, (((1,), (1,)), ((), ())), preferred_element_type=jnp.float32)
                for part in (upper, lower)
            )
            for s in range(spots):
                g_ref[s, :mine] = value[s * mine : (s + 1) * mine, :]
                g_ref[s, mine:] = cross[s * mine : (s + 1) * mine, :]

        @pl.when(i == 0)
        def _():
            gene = lax.broadcasted_iota(jnp.int32, (genes, width), 0)
            position = spot[0] * width + lax.broadcasted_iota(jnp.int32, (genes, width), 1)
            low, high = jnp.zeros_like(gene), jnp.zeros_like(gene)
            for g in range(genes):
                low = jnp.where(gene == g, first[g], low)
                high = jnp.where(gene == g, last[g], high)
            w = w_ref[...].astype(jnp.float32)
            low_w[...] = jnp.where((position >= low) & (position < high), w, 0.0).astype(jnp.bfloat16)
            if copied:
                even[...] = c_ref[...]
            else:
                multiply(even)
            squares()

        if copied:

            @pl.when(i == 1)
            def _():
                multiply(odd)
                store(even, False)
                squares()

        @pl.when((i % 2 == 1) & (i < count) & (i >= (3 if copied else 1)))
        def _():
            multiply(odd)
            store(even, True)
            squares()

        @pl.when((i % 2 == 0) & (i < count) & (i > 0))
        def _():
            multiply(even)
            store(odd, True)
            squares()

        @pl.when(i == count)
        def _():
            store(odd if count % 2 == 0 else even, True)

    whole = lambda i, *_: (0, 0)
    in_specs = [
        pl.BlockSpec((depth, band), lambda i, place, *_: (0, at(now(i), place))),
        pl.BlockSpec((depth, width), whole),
        pl.BlockSpec((genes, width), whole),
    ]
    operands = [place[0], place[2], place[1], begin, end, phenotypes, dosages, weights]
    aliases = {}
    if copied:
        in_specs.append(pl.BlockSpec((band, width), whole))
        operands.append(far)
    if earlier is not None:
        aliases = {len(operands) + k: k for k in range(len(earlier))}
        in_specs += [pl.BlockSpec(memory_space=pl.ANY)] * len(earlier)
        operands += earlier
    return pl.pallas_call(
        body,
        grid_spec=pltpu.PrefetchScalarGridSpec(
            num_scalar_prefetch=5,
            grid=(count + 1,),
            in_specs=in_specs,
            out_specs=[pl.BlockSpec((1, rest, width), lambda i, place, *_: (at(before(i), place), 0, 0))] * ranks
            + [
                pl.BlockSpec((1, band), lambda i, place, *_: (0, at(now(i), place))),
                pl.BlockSpec((spots, 2 * mine, band), lambda i, place, *_: (0, 0, at(before(i), place))),
                pl.BlockSpec(
                    (1, ranks, CUT, width), lambda i, *_: (jnp.clip(i - 1 - count + kept, 0, kept - 1), 0, 0, 0)
                ),
            ],
            scratch_shapes=[
                pltpu.VMEM((band, width), jnp.float32),
                pltpu.VMEM((band, width), jnp.float32),
                pltpu.VMEM((genes, width), jnp.bfloat16),
            ],
        ),
        out_shape=[jax.ShapeDtypeStruct((groups, rest, width), jnp.float32)] * ranks
        + [
            jax.ShapeDtypeStruct((1, traits), jnp.float32),
            jax.ShapeDtypeStruct((spots, 2 * mine, depth), jnp.float32),
            jax.ShapeDtypeStruct((kept, ranks, CUT, width), jnp.float32),
        ],
        input_output_aliases=aliases,
        compiler_params=pltpu.CompilerParams(vmem_limit_bytes=56 * 2**20),
        cost_estimate=pl.CostEstimate(
            flops=2 * depth * band * count * width, bytes_accessed=2 * depth * (traits + width), transcendentals=0
        ),
        name="products",
    )(*operands)


def small_sums(parts, trait_sq, dose_sq, groups):
    spots, rows, _ = parts.shape
    mine = rows // 2
    band = trait_sq.shape[1] // groups
    width = dose_sq.shape[1]

    def body(g_ref, t_ref, q_ref, o_ref):
        total = g_ref[0]
        for s in range(1, spots):
            total = total + g_ref[s]
        predicted = total[:mine]
        squares = jnp.sum(predicted * predicted, axis=1, keepdims=True)
        o_ref[...] = jnp.zeros_like(o_ref)
        for g in range(groups):
            cols = slice(g * band, (g + 1) * band)
            o_ref[8 * g : 8 * g + mine, :band] = total[mine:, cols]
            o_ref[8 * g + 2 : 8 * g + 3, :band] = t_ref[:, cols]
            o_ref[8 * g + 3 : 8 * g + 4, :] = q_ref[...]
            o_ref[8 * g + 4 : 8 * g + 4 + mine, :] = jnp.broadcast_to(squares, (mine, width))

    return pl.pallas_call(
        body,
        out_shape=jax.ShapeDtypeStruct((8 * groups, width), jnp.float32),
        compiler_params=pltpu.CompilerParams(vmem_limit_bytes=8 * 2**20),
        cost_estimate=pl.CostEstimate(flops=10**6, bytes_accessed=10**6, transcendentals=0),
        name="small_sums",
    )(parts, trait_sq, dose_sq)


def joined(pieces, extras):
    groups, rest, width = pieces[0].shape
    count = len(pieces)

    def body(*refs):
        o_ref = refs[-1]
        total = refs[0][...]
        for ref in refs[1:count]:
            total = total + ref[...]
        o_ref[:, :rest, :] = total
        small = refs[count][...]
        for ref in refs[count + 1 : -1]:
            small = small + ref[...]
        for g in range(groups):
            o_ref[g, rest:, :] = small[8 * g : 8 * g + 8, :]

    return pl.pallas_call(
        body,
        out_shape=jax.ShapeDtypeStruct((groups, rest + 8, width), jnp.float32),
        compiler_params=pltpu.CompilerParams(vmem_limit_bytes=16 * 2**20),
        cost_estimate=pl.CostEstimate(
            flops=count * pieces[0].size, bytes_accessed=20 * pieces[0].size, transcendentals=0
        ),
        name="joined",
    )(*pieces, *extras)


def device_part(dosages, phenotypes, gene_weights, gene_start, gene_end):
    _, gene_count = gene_weights.shape
    groups, ranks, spots = (lax.axis_size(a) for a in ("samp_0", "samp_1", "pos"))
    z, y, x = (lax.axis_index(a) for a in ("samp_0", "samp_1", "pos"))
    samples = dosages.shape[0] * groups * ranks
    traits = phenotypes.shape[1]
    band = traits // groups
    own = band // ranks
    rest = own - CUT
    mine = gene_count // spots
    forward = lax.rem(x, 2) == 0

    place = (z.reshape(1), y.reshape(1), x.reshape(1))
    far, z_far, dose_sq = far_product(place, phenotypes, dosages, groups, ranks)
    z_in = parted(z_far, "samp_0")
    rest_of = (place, phenotypes, dosages, gene_weights.T, gene_start, gene_end, groups, ranks, spots)
    *earlier, z_own = products((3, -3, 2, -2), None, None, *rest_of)
    *earlier, z_last = products((4, 1, -1, 0), far, earlier, *rest_of)
    y0, y1, y2, y3, trait_sq, partial_value = earlier
    arrived = [shifted(y2, "samp_1", 2), shifted(y1, "samp_1", 1), shifted(y3, "samp_1", -1)]
    parts = swapped(partial_value, "pos")

    nothing = jnp.zeros_like(z_in)
    z_right = shifted(z_own[0] + jnp.where(forward, z_in, nothing), "samp_0", 1)
    z_left = shifted(z_own[1] + jnp.where(forward, nothing, z_in), "samp_0", -1)

    extra = small_sums(parts, trait_sq, dose_sq, groups)
    extras = [extra] + [shifted(extra, "samp_1", k) for k in (2, 1, 3)]

    for mid in (z_own[2:], z_last):
        z_right, z_left = lax.optimization_barrier((z_right, z_left))
        z_right = shifted(mid[0] + z_right, "samp_0", 1)
        z_left = shifted(mid[1] + z_left, "samp_0", -1)

    second = joined([y0] + arrived, extras)
    second = swapped(second, "samp_0")
    second = second.sum(axis=0)

    first = z_last[2] + z_right + z_left

    def for_rank(k):
        return lax.dynamic_index_in_dim(first, lax.rem(y + k, ranks), 0, False)

    first = for_rank(0) + sum(shifted(for_rank(k), "samp_1", k) for k in (2, 1, 3))

    small = second[rest:]
    mean_dose = small[3] / samples
    mean_pred = small[4 : 4 + mine, 0] / samples
    here = lax.dynamic_slice_in_dim(small[: mine + 1], y * own, own, 1)
    gene_cross = here[:mine].T
    mean_trait = here[mine] / samples
    marginal = jnp.concatenate([first, second[:rest]], 0)
    variant_z = marginal / jnp.sqrt(
        samples * (mean_trait[:, None] + EPSILON) * (mean_dose[None, :] + EPSILON)
    )
    gene_z = gene_cross / jnp.sqrt(
        samples * (mean_trait[:, None] + EPSILON) * (mean_pred[None, :] + EPSILON)
    )
    return (variant_z, gene_z)


def solution(mesh):
    finer = Mesh(mesh.devices.reshape(8, 4, mesh.shape["pos"]), ("samp_0", "samp_1", "pos"))
    in_specs = (P(SAMP, "pos"), P(SAMP, None), P("pos", None), P(), P())
    out_specs = (P(SAMP, "pos"), P(SAMP, "pos"))
    return jax.shard_map(device_part, mesh=finer, in_specs=in_specs, out_specs=out_specs, check_vma=False)
```
